32 devices in a mesh: band: 8 (over z, core), grid: 4 (over y, x).
Axes of the slice: x: 2, y: 2, z: 4, core: 2. Of those that a mesh axis runs over, the one named last changes fastest.
Arguments:
- orbitals: bfloat16 [16, 192, 192, 192], P('band', 'grid'), may hold values from -6 to 6
- plan: int32 [2, 16], P(None, 'band'), may hold values from 0 to 1
Outputs:
- exchange_image: bfloat16 [16, 192, 192, 192], P('band', 'grid')
The draws below stay inside these ranges and needn't reach their ends.
Inputs may be any that keep to these rules, and one draw needn't show every extreme that they name: plan[s, i] is the position, within the partner group of band i at shift s + 1, of the band that band i pairs with.
All inputs are finite; a program needn't handle non-finite values.
Results may differ from the reference program's by a relative error of at most 0.0095.
Values may be sent and summed in bfloat16 or wider, within the bound.
A program may use at most 192 MiB of HBM per device.

```python
import jax
import jax.numpy as jnp
from jax import lax

NG = 192
B_DEV = 2
SHIFTS = 2
BANDS = 16
N_BAND = 8


def with_ends(entries, key, smallest, high):
    shape = entries.shape
    spot = [jax.random.randint(jax.random.fold_in(key, axis), (), 0, shape[axis]) for axis in range(len(shape))]
    entries = entries.at[tuple(spot)].set(smallest)
    longest = shape.index(max(shape))
    spot[longest] = (spot[longest] + 1) % shape[longest]
    return entries.at[tuple(spot)].set(high)


def level_of(key, dims, split, least, top_value):
    loudness = 1.0
    for dim, shards_of in split:
        draws = jax.random.uniform(jax.random.fold_in(jax.random.fold_in(key, 6), dim), (shards_of,), jnp.float32, least / len(split), top_value / len(split))
        loudness = loudness * jnp.repeat(jnp.exp(draws), dims[dim] // shards_of).reshape((-1,) + (1,) * (len(dims) - 1 - dim))
    return loudness


def noise(rng, dims, deviation, reach, shards=(), held_as=jnp.bfloat16):
    values = jax.random.normal(rng, dims, jnp.float32) * deviation
    if len(shards) > 0:
        values = level_of(rng, dims, shards, -0.22, 0.18) * values
    return jnp.clip(values, min=-reach, max=reach).astype(held_as)


def setup_inputs(seed: int = 0) -> dict:
    key_list = jax.random.split(jax.random.key(seed), 3)
    return {
        "orbitals": noise(key_list[0], (BANDS, NG, NG, NG), 1.0, 6.0, ((0, 8), (1, 4))),
        "plan": with_ends(jax.random.randint(key_list[1], (SHIFTS, BANDS), 0, B_DEV), jax.random.fold_in(key_list[1], 1), 0, B_DEV - 1).astype(jnp.int32),
    }


screening = 0.0005


def sine_table(length):
    counts = jnp.arange(1, length + 1, dtype=jnp.float32)
    return jnp.sin(jnp.pi * counts[:, None] * counts[None, :] / (length + 1)).astype(jnp.bfloat16)


def eigen_line(modes, length):
    return 2.0 - 2.0 * jnp.cos(jnp.pi * modes / (length + 1))


def rounded(values):
    return lax.optimization_barrier(values.astype(jnp.bfloat16)).astype(jnp.float32)


def solve(density, table, kernel):
    high = lax.Precision.HIGHEST
    field = density.astype(jnp.float32)
    section = rounded(jnp.einsum("xyz,kz->xyk", field, table, precision=high))
    section = rounded(jnp.einsum("xyz,ky->xkz", section, table, precision=high))
    spectrum = jnp.einsum("xyz,kx->kyz", section, table, precision=high)
    section = rounded(spectrum * kernel)
    section = rounded(jnp.einsum("xyz,kx->kyz", section, table, precision=high))
    section = rounded(jnp.einsum("xyz,ky->xkz", section, table, precision=high))
    return jnp.einsum("xyz,kz->xyk", section, table, precision=high)


def reference(orbitals, plan):
    band_count = orbitals.shape[0]
    length = orbitals.shape[1]
    per_group = band_count // N_BAND
    table = sine_table(length).astype(jnp.float32)
    modes = jnp.arange(1, length + 1, dtype=jnp.float32)
    line = eigen_line(modes, length)
    kernel = (2.0 / (length + 1)) ** 3 / (line[:, None, None] + line[None, :, None] + line[None, None, :] + screening)
    own_sums = jnp.zeros(orbitals.shape, jnp.float32)
    for offset in range(1, SHIFTS + 1):
        def step(carry, index):
            own_acc, partner_acc = carry
            group = index // per_group
            partner = (((group + offset) % N_BAND) * per_group + plan[offset - 1, index]).astype(jnp.int32)
            first_band = orbitals[index].astype(jnp.float32)
            second_band = orbitals[partner].astype(jnp.float32)
            density = (first_band * second_band).astype(jnp.bfloat16)
            potential = solve(density, table, kernel)
            own_acc = own_acc.at[index].add(potential * second_band)
            partner_acc = partner_acc.at[partner].add(potential * first_band)
            return (own_acc, partner_acc), None

        partner_zero = jnp.zeros(orbitals.shape, jnp.float32)
        (own_sums, partner_sums), _ = lax.scan(step, (own_sums, partner_zero), jnp.arange(band_count, dtype=jnp.int32))
        own_sums = own_sums + rounded(partner_sums)
    return (-own_sums).astype(jnp.bfloat16)
```

```python
import jax
import jax.numpy as jnp
from jax import lax
from jax.sharding import PartitionSpec as P

CHUNKS = 4
PACK = True

screening = 0.0005


def routed(block, axis, target):
    return lax.ppermute(block, axis, [(i, target(i)) for i in range(lax.axis_size(axis))])


def packed_send(block, axis, target):
    parts = block.shape[0]
    length = block.shape[-1]
    if not PACK or length % 128 == 0 or (2 * length) % 128 or parts % 2:
        return routed(block, axis, target)
    half = parts // 2
    wide = jnp.concatenate([block[:half], block[half:]], axis=-1)
    got = routed(wide, axis, target)
    return jnp.concatenate([got[..., :length], got[..., length:]], axis=0)


def sine_table(length):
    counts = jnp.arange(1, length + 1, dtype=jnp.float32)
    return jnp.sin(jnp.pi * counts[:, None] * counts[None, :] / (length + 1)).astype(jnp.bfloat16)


def eigen_line(modes, length):
    return 2.0 - 2.0 * jnp.cos(jnp.pi * modes / (length + 1))


def shards(orbitals, plan):
    per_group, planes, _, length = orbitals.shape
    grid = lax.axis_size("grid")
    bands = lax.axis_size("band")
    me = lax.axis_index("grid")
    even = lax.axis_index("band") % 2 == 0
    columns = length // grid
    chunks = CHUNKS if planes % CHUNKS == 0 else 1
    width = planes // chunks

    def peer(i, r):
        return i ^ r if grid & (grid - 1) == 0 else (r - i) % grid

    def to_peer(block, r):
        return block if r == 0 else packed_send(block, "grid", lambda i: peer(i, r))

    sines = sine_table(length)
    peers = jnp.stack([jnp.asarray(peer(me, r), jnp.int32) for r in range(grid)])
    by_column = (peers[:, None] * columns + jnp.arange(columns)[None, :]).reshape(-1)
    by_plane = (
        peers[None, :, None] * planes
        + (jnp.arange(chunks) * width)[:, None, None]
        + jnp.arange(width)[None, None, :]
    ).reshape(-1)
    sines_y = sines[by_column]
    sines_x = sines[by_plane]

    mine = me if grid & (grid - 1) == 0 else peer(me, 0)
    modes = jnp.arange(1, length + 1, dtype=jnp.float32)
    local_modes = (mine * columns + jnp.arange(1, columns + 1, dtype=jnp.int32)).astype(jnp.float32)
    along_full = eigen_line(modes, length)
    along_local = eigen_line(local_modes, length)
    kernel = (2.0 / (length + 1)) ** 3 / (
        along_full[:, None, None]
        + along_local[None, :, None]
        + along_full[None, None, :]
        + screening
    )

    def pick(block, s):
        rows = []
        for i in range(per_group):
            row = block[0]
            for j in range(1, per_group):
                row = jnp.where(plan[s, i] == j, block[j], row)
            rows.append(row)
        return jnp.stack(rows)

    own, picked = [], []
    arrived = []
    for c in range(chunks):
        block = orbitals[:, c * width : (c + 1) * width]
        far = packed_send(block, "band", lambda i: (i - 2) % bands)
        near = packed_send(jnp.where(even, far, block), "band", lambda i: i ^ 1)
        chosen = jnp.concatenate([pick(near, 0), pick(far, 1)])
        both = jnp.concatenate([block, block])
        density = (both.astype(jnp.float32) * chosen.astype(jnp.float32)).astype(jnp.bfloat16)
        section = jnp.dot(density, sines, preferred_element_type=jnp.float32).astype(jnp.bfloat16)
        section = jnp.einsum(
            "pxyz,ky->pxkz", section, sines_y, preferred_element_type=jnp.float32
        ).astype(jnp.bfloat16)
        own.append(block)
        picked.append(chosen)
        for r in range(grid):
            arrived.append(to_peer(section[:, :, r * columns : (r + 1) * columns], r))

    pencils = jnp.concatenate(arrived, axis=1)
    spectrum = jnp.einsum("pxyz,xk->pkyz", pencils, sines_x, preferred_element_type=jnp.float32)
    scaled = (spectrum * kernel).astype(jnp.bfloat16)
    inverse = jnp.einsum(
        "pkyz,xk->pxyz", scaled, sines_x, preferred_element_type=jnp.float32
    ).astype(jnp.bfloat16)

    results = []
    for c in range(chunks):
        slabs = []
        for r in range(grid):
            start = (c * grid + r) * width
            slabs.append(to_peer(inverse[:, start : start + width], r))
        slab = jnp.concatenate(slabs, axis=2)
        slab = jnp.einsum(
            "pxyz,yk->pxkz", slab, sines_y, preferred_element_type=jnp.float32
        ).astype(jnp.bfloat16)
        potential = jnp.dot(slab, sines, preferred_element_type=jnp.float32)
        block = own[c].astype(jnp.float32)
        terms = potential * picked[c].astype(jnp.float32)
        total = terms[:per_group] + terms[per_group:]

        def partner_sum(s):
            weighted = potential[s * per_group : (s + 1) * per_group] * block
            return jnp.stack(
                [
                    sum(jnp.where(plan[s, i] == j, weighted[i], 0.0) for i in range(per_group))
                    for j in range(per_group)
                ]
            )

        swapped = packed_send(partner_sum(0).astype(jnp.bfloat16), "band", lambda i: i ^ 1)
        swapped = swapped.astype(jnp.float32)
        outgoing = partner_sum(1) + jnp.where(even, swapped, 0.0)
        returned = packed_send(outgoing.astype(jnp.bfloat16), "band", lambda i: (i + 2) % bands)
        total = total + jnp.where(even, 0.0, swapped) + returned.astype(jnp.float32)
        results.append((-total).astype(jnp.bfloat16))
    return jnp.concatenate(results, axis=1)


def solution(mesh):
    return jax.shard_map(
        shards,
        mesh=mesh,
        in_specs=(P("band", "grid", None, None), P(None, "band")),
        out_specs=P("band", "grid", None, None),
        check_vma=False,
    )
```
